16 devices in a mesh: dp: 1, tp: 16 (over x, y, z, core).
Axes of the slice: x: 2, y: 2, z: 2, core: 2. Of those that a mesh axis runs over, the one named last changes fastest.
Arguments:
- x: bfloat16 [64, 2048], P('dp')
- k_cache: bfloat16 [64, 4096, 16, 128], P('dp', None, 'tp')
- v_cache: bfloat16 [64, 4096, 16, 128], P('dp', None, 'tp')
- gain_a: bfloat16 [2048], replicated
- wq: bfloat16 [2048, 2048], P(None, 'tp')
- wo: bfloat16 [2048, 2048], P('tp')
- gain_m: bfloat16 [2048], replicated
- w_gate: bfloat16 [2048, 8192], P(None, 'tp')
- w_up: bfloat16 [2048, 8192], P(None, 'tp')
- w_down: bfloat16 [8192, 2048], P('tp')
Outputs:
- output: bfloat16 [64, 2048], P('dp')
All inputs are finite; a program needn't handle non-finite values.
Results may differ from the reference program's by a relative error of at most 0.017.
Values are sent between devices in bfloat16 or wider.
A program may use at most 2 GiB of HBM per device.

```python
import jax
import jax.numpy as jnp
from jax import lax

BATCH = 64
CACHE = 4096
D = 2048
HEADS = 16
KV_HEADS = 16
HEAD = 128
FF = 8192
THETA = 10000


def setup_inputs(seed: int = 0, part: int = 0) -> dict:
    kx, kc, kw, kn, kq, ko, km, kg, ku, kd = jax.random.split(jax.random.key(seed), 10)
    kx, kc, kw = (jax.random.fold_in(k, part) for k in (kx, kc, kw))

    def weights(key, rows, columns):
        return jax.random.normal(key, (rows, columns), jnp.float32) * rows**-0.5

    drawn = {
        "x": jax.random.normal(kx, (BATCH, D), jnp.float32),
        "k_cache": 2 * jax.random.normal(kc, (BATCH, CACHE, KV_HEADS, HEAD), jnp.float32),
        "v_cache": 4 * jax.random.normal(kw, (BATCH, CACHE, KV_HEADS, HEAD), jnp.float32),
        "gain_a": 1 + 0.1 * jax.random.normal(kn, (D,), jnp.float32),
        "wq": 2 * weights(kq, D, HEADS * HEAD),
        "wo": weights(ko, HEADS * HEAD, D),
        "gain_m": 1 + 0.1 * jax.random.normal(km, (D,), jnp.float32),
        "w_gate": weights(kg, D, FF),
        "w_up": weights(ku, D, FF),
        "w_down": 2 * weights(kd, FF, D),
    }
    return {k: v.astype(jnp.bfloat16) for k, v in drawn.items()}


def normed(x, gain):
    wide = x.astype(jnp.float32)
    scale = lax.rsqrt(jnp.mean(wide * wide, -1, keepdims=True) + 1e-6)
    return (wide * scale * gain.astype(jnp.float32)).astype(jnp.bfloat16)


def turned(t, place, theta):
    half = t.shape[-1] // 2
    angle = place.astype(jnp.float32)[:, None] * theta ** (-jnp.arange(half, dtype=jnp.float32) / half)
    cos, sin = jnp.cos(angle)[:, None], jnp.sin(angle)[:, None]
    a, b = t[..., :half].astype(jnp.float32), t[..., half:].astype(jnp.float32)
    return jnp.concatenate([a * cos - b * sin, b * cos + a * sin], -1).astype(jnp.bfloat16)


def matmul(a, w):
    return jnp.dot(a, w, preferred_element_type=jnp.float32).astype(jnp.bfloat16)


def einsum(form, a, b):
    return jnp.einsum(form, a.astype(jnp.float32), b.astype(jnp.float32))


def seen_by(a, wq, k_cache, v_cache, head, theta):
    batch, cache, kv_heads = k_cache.shape[:3]
    place = jnp.full((batch,), cache - 1)
    q = turned(matmul(a, wq).reshape(batch, -1, head), place, theta).reshape(batch, kv_heads, -1, head)
    scores = einsum("bgsd,bugd->bgsu", q, k_cache) * head**-0.5
    weights = jax.nn.softmax(scores, -1).astype(jnp.bfloat16)
    return einsum("bgsu,bugd->bgsd", weights, v_cache).astype(jnp.bfloat16).reshape(batch, -1)


def hidden_of(b, w_gate, w_up):
    gate = jnp.dot(b, w_gate, preferred_element_type=jnp.float32)
    up = jnp.dot(b, w_up, preferred_element_type=jnp.float32)
    return (jax.nn.silu(gate) * up).astype(jnp.bfloat16)


def reference(x, k_cache, v_cache, gain_a, wq, wo, gain_m, w_gate, w_up, w_down):
    seen = seen_by(normed(x, gain_a), wq, k_cache, v_cache, HEAD, THETA)
    h = (x.astype(jnp.float32) + jnp.dot(seen, wo, preferred_element_type=jnp.float32)).astype(jnp.bfloat16)
    hidden = hidden_of(normed(h, gain_m), w_gate, w_up)
    return (h.astype(jnp.float32) + jnp.dot(hidden, w_down, preferred_element_type=jnp.float32)).astype(jnp.bfloat16)
```

```python
import functools

import jax
import jax.numpy as jnp
import numpy as np
from jax import lax
from jax.experimental import pallas as pl
from jax.experimental.pallas import tpu as pltpu
from jax.sharding import PartitionSpec as P

HEAD = 128
THETA = 10000
EPS = 1e-6
N = 16
BATCH = 64
CACHE = 4096
D = 2048
FF = 512
GROUP = 8
PAIRS = GROUP // 2
GROUPS = BATCH // GROUP
TILE = 256
TILES = CACHE // TILE
AHEAD = 8
SLOTS = 8
F32, BF16 = jnp.float32, jnp.bfloat16


def other(me, k):
    bits = [((me // 2**i) % 2 + (k >> i & 1)) % 2 * 2**i for i in range(4)]
    return bits[0] + bits[1] + bits[2] + bits[3]


ORDER = sorted(range(1, N), key=lambda k: -(bin(k >> 1).count("1") * 2 + (k & 1)))


def kernel(x_hbm, k_hbm, v_hbm, ga_hbm, wq_hbm, wo_hbm, gm_hbm, wg_hbm, wu_hbm, wd_hbm, rot_hbm, o_ref,
           x_v, ga_v, gm_v, wq_v, wo_v, wg_v, wu_v, wd_v, rot_v, a_v, q_v, s_v, p_v, seen_v, kbuf, vbuf,
           send_a, recv_a, h_all, send_m, recv_m, wsem, ksem, vsem, send_sem, recv_sem):
    me = lax.axis_index("tp")

    small = [pltpu.make_async_copy(src, dst, wsem.at[i]) for i, (src, dst) in enumerate((
        (x_hbm, x_v), (ga_hbm, ga_v), (wq_hbm, wq_v), (rot_hbm, rot_v)))]
    later = [pltpu.make_async_copy(src, dst, wsem.at[4 + i]) for i, (src, dst) in enumerate((
        (wo_hbm, wo_v), (gm_hbm, gm_v), (wg_hbm, wg_v), (wu_hbm, wu_v), (wd_hbm, wd_v)))]

    def pair_copy(hbm, buf, sem, pair):
        slot = lax.rem(pair, SLOTS)
        return pltpu.make_async_copy(hbm.at[pl.ds(pair * 2, 2)], buf.at[slot], sem.at[slot])

    def start_unit(u):
        group, phase, p = u // (2 * PAIRS), lax.rem(u // PAIRS, 2), lax.rem(u, PAIRS)
        pair = group * PAIRS + p

        @pl.when(jnp.logical_and(phase == 0, group < GROUPS))
        def _():
            pair_copy(k_hbm, kbuf, ksem, pair).start()

        @pl.when(jnp.logical_and(phase == 1, group < GROUPS))
        def _():
            pair_copy(v_hbm, vbuf, vsem, pair).start()

    for copy in small:
        copy.start()
    lax.fori_loop(0, AHEAD, lambda u, _: (start_unit(u), 0)[1], 0)

    barrier = pltpu.get_barrier_semaphore()
    for k in range(1, N):
        pl.semaphore_signal(barrier, inc=1, device_id={"tp": other(me, k)}, device_id_type=pl.DeviceIdType.MESH)

    def norm_into(columns, gain_v):
        total = jnp.zeros((BATCH, HEAD), F32)
        for c in range(N):
            wide = columns(c).astype(F32)
            total += wide * wide
        scale = lax.rsqrt(jnp.sum(total, -1, keepdims=True) / D + EPS)
        gain = gain_v[...].astype(F32)
        for c in range(N):
            a_v[:, c * HEAD:(c + 1) * HEAD] = (columns(c).astype(F32) * scale * gain[c:c + 1, :]).astype(BF16)

    for copy in small:
        copy.wait()
    norm_into(lambda c: x_v[:, c * HEAD:(c + 1) * HEAD], ga_v)
    q = jnp.dot(a_v[...], wq_v[...], preferred_element_type=F32).astype(BF16).astype(F32)
    q = q * rot_v[0:1, :] + pltpu.roll(q, HEAD // 2, 1) * rot_v[1:2, :]
    q_v[...] = q.astype(BF16).astype(F32)

    for copy in later:
        copy.start()

    rows = lax.broadcasted_iota(jnp.int32, (GROUP, HEAD), 0)

    def group_step(g, _):
        query = q_v[pl.ds(pl.multiple_of(g * GROUP, GROUP), GROUP), :]
        s_v[...] = jnp.zeros_like(s_v)

        def score_pair(p, _):
            pair = g * PAIRS + p
            slot = lax.rem(pair, SLOTS)
            pair_copy(k_hbm, kbuf, ksem, pair).wait()
            lhs = jnp.concatenate([jnp.where(rows == 2 * p, query, 0.0), jnp.where(rows == 2 * p + 1, query, 0.0)], 1).astype(BF16)
            for j in range(TILES):
                keys = slice(j * TILE, (j + 1) * TILE)
                rhs = jnp.concatenate([kbuf[slot, 0, keys, :], kbuf[slot, 1, keys, :]], 1)
                s_v[:, keys] += lax.dot_general(lhs, rhs, (((1,), (1,)), ((), ())), preferred_element_type=F32)
            start_unit(g * 2 * PAIRS + p + AHEAD)
            return 0

        lax.fori_loop(0, PAIRS, score_pair, 0)

        scores = s_v[...] * HEAD**-0.5
        e = jnp.exp(scores - jnp.max(scores, -1, keepdims=True))
        p_v[...] = (e * (1.0 / jnp.sum(e, -1, keepdims=True))).astype(BF16)

        def value_pair(p, seen):
            pair = g * PAIRS + p
            slot = lax.rem(pair, SLOTS)
            pair_copy(v_hbm, vbuf, vsem, pair).wait()
            acc = [jnp.zeros((GROUP, 2 * HEAD), F32) for _ in range(2)]
            for j in range(TILES):
                keys = slice(j * TILE, (j + 1) * TILE)
                rhs = jnp.concatenate([vbuf[slot, 0, keys, :], vbuf[slot, 1, keys, :]], 1)
                acc[j % 2] += jnp.dot(p_v[:, keys], rhs, preferred_element_type=F32)
            out = acc[0] + acc[1]
            start_unit(g * 2 * PAIRS + PAIRS + p + AHEAD)
            return jnp.where(rows == 2 * p, out[:, :HEAD], jnp.where(rows == 2 * p + 1, out[:, HEAD:], seen))

        seen = lax.fori_loop(0, PAIRS, value_pair, jnp.zeros((GROUP, HEAD), F32))
        seen_v[pl.ds(pl.multiple_of(g * GROUP, GROUP), GROUP), :] = seen
        return 0

    lax.fori_loop(0, GROUPS, group_step, 0)

    for copy in later:
        copy.wait()
    pl.semaphore_wait(barrier, N - 1)

    mine = pl.ds(pl.multiple_of(me * HEAD, HEAD), HEAD)

    def exchange(phase, source, target):
        copies = {}
        for k in ORDER:
            peer = other(me, k)
            copies[k] = pltpu.make_async_remote_copy(
                src_ref=source(peer), dst_ref=target(k), send_sem=send_sem.at[phase, k], recv_sem=recv_sem.at[phase, k],
                device_id={"tp": peer}, device_id_type=pl.DeviceIdType.MESH)
            copies[k].start()
        return copies

    def summed(phase, left, w_v, send, recv, base):
        for c in range(0, N, 2):
            term = jnp.dot(left, w_v[:, c * HEAD:(c + 2) * HEAD], preferred_element_type=F32).astype(BF16)
            send[c] = term[:, :HEAD]
            send[c + 1] = term[:, HEAD:]
        copies = exchange(phase, lambda peer: send.at[peer], lambda k: recv.at[k])
        total = base + jnp.dot(left, w_v[:, mine], preferred_element_type=F32)
        for k in reversed(ORDER):
            copies[k].wait_recv()
            total += recv[k].astype(F32)
        return total, copies

    h, sent = summed(0, seen_v[...].astype(BF16), wo_v, send_a, recv_a, x_v[:, mine].astype(F32))
    h_all[me] = h.astype(BF16)
    spread = exchange(1, lambda peer: h_all.at[me], lambda k: h_all.at[me])

    def arrived(phase, k, ref):
        peer = other(me, k)
        pltpu.make_async_remote_copy(
            src_ref=ref(me), dst_ref=ref(peer), send_sem=send_sem.at[phase, k], recv_sem=recv_sem.at[phase, k],
            device_id={"tp": peer}, device_id_type=pl.DeviceIdType.MESH).wait_recv()

    for k in reversed(ORDER):
        arrived(1, k, lambda c: h_all.at[c])
    norm_into(lambda c: h_all[c], gm_v)
    gate = jnp.dot(a_v[...], wg_v[...], preferred_element_type=F32)
    up = jnp.dot(a_v[...], wu_v[...], preferred_element_type=F32)
    hidden = (gate * (1.0 / (1.0 + jnp.exp(-gate))) * up).astype(BF16)
    y, sent_m = summed(2, hidden, wd_v, send_m, recv_m, h_all[me].astype(F32))
    o_ref[:, mine] = y.astype(BF16)
    spread_m = exchange(3, lambda peer: o_ref.at[:, mine], lambda k: o_ref.at[:, mine])
    for k in reversed(ORDER):
        arrived(3, k, lambda c: o_ref.at[:, pl.ds(pl.multiple_of(c * HEAD, HEAD), HEAD)])
    for copies in (sent, spread, sent_m, spread_m):
        for k in ORDER:
            copies[k].wait_send()


def rotary_table():
    half = HEAD // 2
    angle = (CACHE - 1) * THETA ** (-np.arange(half, dtype=np.float64) / half)
    cos, sin = np.cos(angle), np.sin(angle)
    table = np.zeros((8, HEAD), np.float32)
    table[0], table[1] = np.concatenate([cos, cos]), np.concatenate([-sin, sin])
    return table


def solution(mesh):
    def step(x, k_cache, v_cache, gain_a, wq, wo, gain_m, w_gate, w_up, w_down):
        whole = pl.BlockSpec(memory_space=pl.ANY)
        call = pl.pallas_call(
            kernel,
            out_shape=jax.ShapeDtypeStruct((BATCH, D), BF16),
            in_specs=[whole] * 11,
            out_specs=pl.BlockSpec(memory_space=pltpu.VMEM),
            scratch_shapes=[
                pltpu.VMEM((BATCH, D), BF16), pltpu.VMEM((N, HEAD), BF16), pltpu.VMEM((N, HEAD), BF16),
                pltpu.VMEM((D, HEAD), BF16), pltpu.VMEM((HEAD, D), BF16), pltpu.VMEM((D, FF), BF16), pltpu.VMEM((D, FF), BF16),
                pltpu.VMEM((FF, D), BF16), pltpu.VMEM((8, HEAD), F32), pltpu.VMEM((BATCH, D), BF16), pltpu.VMEM((BATCH, HEAD), F32),
                pltpu.VMEM((GROUP, CACHE), F32), pltpu.VMEM((GROUP, CACHE), BF16), pltpu.VMEM((BATCH, HEAD), F32),
                pltpu.VMEM((SLOTS, 2, CACHE, HEAD), BF16), pltpu.VMEM((SLOTS, 2, CACHE, HEAD), BF16),
                pltpu.VMEM((N, BATCH, HEAD), BF16), pltpu.VMEM((N, BATCH, HEAD), BF16), pltpu.VMEM((N, BATCH, HEAD), BF16),
                pltpu.VMEM((N, BATCH, HEAD), BF16), pltpu.VMEM((N, BATCH, HEAD), BF16),
                pltpu.SemaphoreType.DMA((9,)), pltpu.SemaphoreType.DMA((SLOTS,)), pltpu.SemaphoreType.DMA((SLOTS,)),
                pltpu.SemaphoreType.DMA((4, N)), pltpu.SemaphoreType.DMA((4, N)),
            ],
            compiler_params=pltpu.CompilerParams(collective_id=0, has_side_effects=True, vmem_limit_bytes=60 * 2**20),
            name="decode_layer",
        )
        return call(x, k_cache.reshape(BATCH, CACHE, HEAD), v_cache.reshape(BATCH, CACHE, HEAD), gain_a.reshape(N, HEAD), wq, wo,
                    gain_m.reshape(N, HEAD), w_gate, w_up, w_down, jnp.asarray(rotary_table()))

    states, cache, columns, rows_of = P("dp", None), P("dp", None, "tp", None), P(None, "tp"), P("tp", None)
    return jax.shard_map(
        step,
        mesh=mesh,
        in_specs=(states, cache, cache, P(None), columns, rows_of, P(None), columns, columns, rows_of),
        out_specs=states,
        check_vma=False,
    )
```

```python
import functools

import jax
import jax.numpy as jnp
import numpy as np
from jax import lax
from jax.experimental import pallas as pl
from jax.experimental.pallas import tpu as pltpu
from jax.sharding import PartitionSpec as P

HEAD = 128
THETA = 10000
EPS = 1e-6
N = 16
BATCH = 64
CACHE = 4096
D = 2048
FF = 512
GROUP = 4
ROWS = 8
GROUPS = BATCH // GROUP
TILE = 256
TILES = CACHE // TILE
SLOTS = 3
WIDE = D // 2
F32, BF16 = jnp.float32, jnp.bfloat16

PARTS = ((0, 32, 32), (32, 32, 24))
LAST = (14, 15)
PHASES = 4 * len(PARTS) + len(LAST)


def other(me, k):
    bits = [((me // 2**i) % 2 + (k >> i & 1)) % 2 * 2**i for i in range(4)]
    return bits[0] + bits[1] + bits[2] + bits[3]


ORDER = sorted(range(1, N), key=lambda k: -(bin(k >> 1).count("1") * 2 + (k & 1)))


def kernel(x_hbm, k_hbm, v_hbm, ga_hbm, wq_hbm, wo_hbm, gm_hbm, wg_hbm, wu_hbm, wd_hbm, rot_hbm, o_ref,
           x_v, ga_v, gm_v, wq_v, wo_v, wg_v, wu_v, wd_v, rot_v, a_v, q_v, s_v, p_v, seen_v, kbuf, vbuf,
           part_bufs, last_bufs, wsem, ksem, vsem, send_sem, recv_sem):
    me = lax.axis_index("tp")
    peers = {k: other(me, k) for k in range(1, N)}
    mine = pl.ds(pl.multiple_of(me * HEAD, HEAD), HEAD)

    small = [pltpu.make_async_copy(src, dst, wsem.at[i]) for i, (src, dst) in enumerate((
        (x_hbm, x_v), (ga_hbm, ga_v), (wq_hbm, wq_v), (rot_hbm, rot_v)))]
    middle = [pltpu.make_async_copy(src, dst, wsem.at[7 + i]) for i, (src, dst) in enumerate(((wo_hbm, wo_v), (gm_hbm, gm_v)))]
    later = [pltpu.make_async_copy(src, dst, wsem.at[4 + i]) for i, (src, dst) in enumerate((
        (wg_hbm, wg_v), (wu_hbm, wu_v), (wd_hbm, wd_v)))]

    def keys_copy(g):
        slot = lax.rem(g, SLOTS)
        return pltpu.make_async_copy(k_hbm.at[pl.ds(g * GROUP, GROUP)], kbuf.at[slot], ksem.at[slot])

    def values_copy(g):
        slot = lax.rem(g, SLOTS)
        return pltpu.make_async_copy(v_hbm.at[pl.ds(g * GROUP, GROUP)], vbuf.at[slot], vsem.at[slot])

    for copy in small:
        copy.start()
    keys_copy(0).start()
    keys_copy(1).start()
    values_copy(0).start()
    keys_copy(2).start()
    values_copy(1).start()

    barrier = pltpu.get_barrier_semaphore()
    for k in range(1, N):
        pl.semaphore_signal(barrier, inc=1, device_id={"tp": peers[k]}, device_id_type=pl.DeviceIdType.MESH)

    def norm_into(first, rows, columns, gain_v):
        total = jnp.zeros((rows, HEAD), F32)
        for c in range(N):
            wide = columns(c).astype(F32)
            total += wide * wide
        scale = lax.rsqrt(jnp.sum(total, -1, keepdims=True) / D + EPS)
        gain = gain_v[...].astype(F32)
        for c in range(N):
            a_v[first:first + rows, c * HEAD:(c + 1) * HEAD] = (columns(c).astype(F32) * scale * gain[c:c + 1, :]).astype(BF16)

    for copy in small:
        copy.wait()
    norm_into(0, BATCH, lambda c: x_v[:, c * HEAD:(c + 1) * HEAD], ga_v)
    q = jnp.dot(a_v[...], wq_v[...], preferred_element_type=F32).astype(BF16).astype(F32)
    q = q * rot_v[0:1, :] + pltpu.roll(q, HEAD // 2, 1) * rot_v[1:2, :]
    q = q.astype(BF16).astype(F32)
    for g in range(GROUPS):
        q_v[g, :GROUP] = q[g * GROUP:(g + 1) * GROUP]

    for copy in middle:
        copy.start()

    rows = lax.broadcasted_iota(jnp.int32, (ROWS, HEAD), 0)

    def score(g):
        slot = lax.rem(g, SLOTS)
        query = q_v[g]
        own = [jnp.where(rows == i, query, 0.0) for i in range(GROUP)]
        lhs = [jnp.concatenate(own[i:i + 2], 1).astype(BF16) for i in range(0, GROUP, 2)]
        for j in range(TILES):
            keys = slice(j * TILE, (j + 1) * TILE)
            total = None
            for i in range(0, GROUP, 2):
                rhs = jnp.concatenate([kbuf[slot, i, keys, :], kbuf[slot, i + 1, keys, :]], 1)
                part = lax.dot_general(lhs[i // 2], rhs, (((1,), (1,)), ((), ())), preferred_element_type=F32)
                total = part if total is None else total + part
            s_v[:, keys] = total

    def weigh(g):
        scores = s_v[...] * HEAD**-0.5
        e = jnp.exp(scores - jnp.max(scores, -1, keepdims=True))
        p_v[lax.rem(g, 2)] = (e * (1.0 / jnp.sum(e, -1, keepdims=True))).astype(BF16)

    def gather(g):
        slot, place = lax.rem(g, SLOTS), lax.rem(g, 2)
        seen = jnp.zeros((ROWS, HEAD), F32)
        for i in range(0, GROUP, 2):
            out = None
            for j in range(TILES):
                keys = slice(j * TILE, (j + 1) * TILE)
                rhs = jnp.concatenate([vbuf[slot, i, keys, :], vbuf[slot, i + 1, keys, :]], 1)
                part = jnp.dot(p_v[place, :, keys], rhs, preferred_element_type=F32)
                out = part if out is None else out + part
            seen = jnp.where(rows == i, out[:, :HEAD], jnp.where(rows == i + 1, out[:, HEAD:], seen))
        seen_v[g] = seen

    def copy(phase, k, source, target):
        return pltpu.make_async_remote_copy(
            src_ref=source, dst_ref=target, send_sem=send_sem.at[phase], recv_sem=recv_sem.at[phase],
            device_id={"tp": peers[k]}, device_id_type=pl.DeviceIdType.MESH)

    def start(phase, source, target):
        for k in ORDER:
            copy(phase, k, source(k), target(k)).start()

    def arrived(phase, size):
        copy(phase, 1, size, size).wait_recv()

    def left_here(phase, size):
        copy(phase, 1, size, size).wait_send()

    def block_of(i, owner):
        first, count, _ = PARTS[i]
        return o_ref.at[first:first + count, pl.ds(pl.multiple_of(owner * HEAD, HEAD), HEAD)]

    def size_of(i, phase):
        first, count, _ = PARTS[i]
        return o_ref.at[first:first + count, :(N - 1) * HEAD] if phase == 3 else part_bufs[i][phase].at[:N - 1]

    def left_of(i, phase):
        first, _, direct = PARTS[i]
        if phase == 0:
            return jnp.concatenate([seen_v[g, :GROUP] for g in range(first // GROUP, (first + direct) // GROUP)], 0).astype(BF16)
        return part_bufs[i][5][...]

    def send_terms(i, phase, w_v):
        left, send = left_of(i, phase), part_bufs[i][phase]
        for c in range(0, N, 2):
            term = jnp.dot(left, w_v[:, c * HEAD:(c + 2) * HEAD], preferred_element_type=F32).astype(BF16)
            send[c] = term[:, :HEAD]
            send[c + 1] = term[:, HEAD:]
        recv = part_bufs[i][phase + 1]
        start(4 * i + phase, lambda k: send.at[peers[k]], lambda k: recv.at[k])

    def finished(i, phase, w_v, base):
        recv = part_bufs[i][phase + 1]
        total = base + jnp.dot(left_of(i, phase), w_v[:, mine], preferred_element_type=F32)
        arrived(4 * i + phase, size_of(i, phase))
        for k in range(1, N):
            total += recv[k].astype(F32)
        return total.astype(BF16)

    def part_a(i):
        send_terms(i, 0, wo_v)

    def part_b(i):
        first, _, direct = PARTS[i]
        part_bufs[i][4][me, :direct] = finished(i, 0, wo_v, x_v[first:first + direct, mine].astype(F32))
        block = part_bufs[i][4].at[me, :PARTS[i][2]]
        start(4 * i + 1, lambda k: block, lambda k: block)

    def part_c(i):
        first, count, direct = PARTS[i]
        h_all, hidden_v = part_bufs[i][4:]
        arrived(4 * i + 1, size_of(i, 1))
        for j, at in enumerate(range(first + direct, first + count, ROWS)):
            h = unpacked(*(first_sum(2 * j + r) for r in range(2)))
            for c in range(N):
                h_all[c, direct + j * ROWS:direct + (j + 1) * ROWS] = h[c // (N // 2)][:, c % (N // 2) * HEAD:(c % (N // 2) + 1) * HEAD].astype(BF16)
        norm_into(first, count, lambda c: h_all[c], gm_v)
        a = a_v[first:first + count]
        gate = jnp.dot(a, wg_v[...], preferred_element_type=F32)
        up = jnp.dot(a, wu_v[...], preferred_element_type=F32)
        hidden_v[...] = (gate * (1.0 / (1.0 + jnp.exp(-gate))) * up).astype(BF16)
        send_terms(i, 2, wd_v)

    def part_d(i):
        block_of(i, me)[...] = finished(i, 2, wd_v, part_bufs[i][4][me].astype(F32))
        start(4 * i + 3, lambda k: block_of(i, me), lambda k: block_of(i, me))

    def part_e(i):
        arrived(4 * i + 3, size_of(i, 3))

    low = lax.broadcasted_iota(jnp.int32, (ROWS, 1), 0) < GROUP

    def packed(left, right):
        return jnp.where(low, left, right)

    def swap(t):
        return pltpu.roll(t, GROUP, 0)

    def last_phase(i):
        return 4 * len(PARTS) + i

    def send_whole(i, left, w_v):
        recv = last_bufs[i]
        for c in range(0, WIDE, 2 * HEAD):
            term = [jnp.dot(left, w_v[:, at:at + 2 * HEAD], preferred_element_type=F32) for at in (c, WIDE + c)]
            recv[me, :, c:c + 2 * HEAD] = packed(*term).astype(BF16)
        start(last_phase(i), lambda k: recv.at[me], lambda k: recv.at[me])

    def added(i, base):
        recv = last_bufs[i]
        arrived(last_phase(i), recv.at[:N - 1])
        total = recv[0].astype(F32)
        for d in range(1, N):
            total += recv[d].astype(F32)
        return (base + total).astype(BF16).astype(F32)

    def last_a(i):
        seen = seen_v[LAST[i]].astype(BF16).astype(F32)
        send_whole(i, (seen + swap(seen)).astype(BF16), wo_v)

    def unpacked(a, b):
        return packed(a, swap(b)), packed(swap(a), b)

    def first_sum(i):
        first = LAST[i] * GROUP // ROWS * ROWS
        x = x_v[first:first + ROWS, :].astype(F32)
        left, right = x[:, :WIDE], x[:, WIDE:]
        return added(i, packed(left, swap(right)) if LAST[i] * GROUP == first else packed(swap(left), right))

    keys_copy(0).wait()
    score(0)
    weigh(0)

    def entered():
        for c in middle:
            c.wait()
        pl.semaphore_wait(barrier, N - 1)

    stages = {
        6: (entered,), 7: (lambda: part_a(0),), 9: (lambda: part_b(0),), 13: (lambda: part_a(1),), 14: (lambda: last_a(0),)}

    def step(g, _):
        keys_copy(g + 1).wait()
        values_copy(g).wait()

        @pl.when(g + 3 < GROUPS)
        def _():
            keys_copy(g + 3).start()

        @pl.when(g + 2 < GROUPS)
        def _():
            values_copy(g + 2).start()

        @pl.when(g + 3 == GROUPS)
        def _():
            for c in later:
                c.start()

        score(g + 1)
        gather(g)
        weigh(g + 1)

        for when, jobs in stages.items():
            @pl.when(g == when)
            def _():
                for job in jobs:
                    job()

        return 0

    lax.fori_loop(0, GROUPS - 1, step, 0)
    values_copy(GROUPS - 1).wait()
    gather(GROUPS - 1)
    last_a(1)
    part_b(1)
    for c in later:
        c.wait()
    part_c(0)
    part_c(1)
    part_d(0)
    part_d(1)
    part_e(0)
    part_e(1)
    for i in range(len(PARTS)):
        for phase in range(4):
            left_here(4 * i + phase, size_of(i, phase))
    for i in range(len(LAST)):
        left_here(last_phase(i), last_bufs[i].at[:N - 1])


def rotary_table():
    half = HEAD // 2
    angle = (CACHE - 1) * THETA ** (-np.arange(half, dtype=np.float64) / half)
    cos, sin = np.cos(angle), np.sin(angle)
    table = np.zeros((8, HEAD), np.float32)
    table[0], table[1] = np.concatenate([cos, cos]), np.concatenate([-sin, sin])
    return table


def solution(mesh):
    def step(x, k_cache, v_cache, gain_a, wq, wo, gain_m, w_gate, w_up, w_down):
        whole = pl.BlockSpec(memory_space=pl.ANY)
        call = pl.pallas_call(
            kernel,
            out_shape=jax.ShapeDtypeStruct((BATCH, D), BF16),
            in_specs=[whole] * 11,
            out_specs=pl.BlockSpec(memory_space=pltpu.VMEM),
            scratch_shapes=[
                pltpu.VMEM((BATCH, D), BF16), pltpu.VMEM((N, HEAD), BF16), pltpu.VMEM((N, HEAD), BF16),
                pltpu.VMEM((D, HEAD), BF16), pltpu.VMEM((HEAD, D), BF16), pltpu.VMEM((D, FF), BF16), pltpu.VMEM((D, FF), BF16),
                pltpu.VMEM((FF, D), BF16), pltpu.VMEM((8, HEAD), F32), pltpu.VMEM((BATCH, D), BF16), pltpu.VMEM((GROUPS, ROWS, HEAD), F32),
                pltpu.VMEM((ROWS, CACHE), F32), pltpu.VMEM((2, ROWS, CACHE), BF16), pltpu.VMEM((GROUPS, ROWS, HEAD), F32),
                pltpu.VMEM((SLOTS, GROUP, CACHE, HEAD), BF16), pltpu.VMEM((SLOTS, GROUP, CACHE, HEAD), BF16),
                [[pltpu.VMEM((N, rows, HEAD), BF16) for rows in (direct, direct, count, count, count)] + [pltpu.VMEM((count, FF), BF16)]
                 for _, count, direct in PARTS],
                [pltpu.VMEM((N, ROWS, WIDE), BF16) for _ in LAST],
                pltpu.SemaphoreType.DMA((9,)), pltpu.SemaphoreType.DMA((SLOTS,)), pltpu.SemaphoreType.DMA((SLOTS,)),
                pltpu.SemaphoreType.DMA((PHASES,)), pltpu.SemaphoreType.DMA((PHASES,)),
            ],
            compiler_params=pltpu.CompilerParams(collective_id=0, has_side_effects=True, vmem_limit_bytes=60 * 2**20),
            name="decode_layer",
        )
        return call(x, k_cache.reshape(BATCH, CACHE, HEAD), v_cache.reshape(BATCH, CACHE, HEAD), gain_a.reshape(N, HEAD), wq, wo,
                    gain_m.reshape(N, HEAD), w_gate, w_up, w_down, jnp.asarray(rotary_table()))

    states, cache, columns, rows_of = P("dp", None), P("dp", None, "tp", None), P(None, "tp"), P("tp", None)
    return jax.shard_map(
        step,
        mesh=mesh,
        in_specs=(states, cache, cache, P(None), columns, rows_of, P(None), columns, columns, rows_of),
        out_specs=states,
        check_vma=False,
    )
```

```python
import functools

import jax
import jax.numpy as jnp
import numpy as np
from jax import lax
from jax.experimental import pallas as pl
from jax.experimental.pallas import tpu as pltpu
from jax.sharding import PartitionSpec as P

HEAD = 128
THETA = 10000
EPS = 1e-6
N = 16
BATCH = 64
CACHE = 4096
D = 2048
FF = 512
GROUP = 4
ROWS = 8
GROUPS = BATCH // GROUP
TILE = 256
TILES = CACHE // TILE
WEIGHTS_AT = 7
SLOTS = 3
F32, BF16 = jnp.float32, jnp.bfloat16

PARTS = ((0, 32), (32, 24))
EARLY = sum(rows for _, rows in PARTS)
LATE = BATCH - EARLY
LATE_AT = 4 * len(PARTS)
OWNERS = ((15, 7, 11, 13), (1, 3, 5, 9))
PART = D // len(OWNERS[0])
PHASES = LATE_AT + 4


def other(me, k):
    bits = [((me // 2**i) % 2 + (k >> i & 1)) % 2 * 2**i for i in range(4)]
    return bits[0] + bits[1] + bits[2] + bits[3]


ORDER = sorted(range(1, N), key=lambda k: -(bin(k >> 1).count("1") * 2 + (k & 1)))


def kernel(x_hbm, k_hbm, v_hbm, ga_hbm, wq_hbm, wo_hbm, gm_hbm, wg_hbm, wu_hbm, wd_hbm, rot_hbm, o_ref,
           x_v, ga_v, gm_v, wq_v, wo_v, wg_v, wu_v, wd_v, rot_v, a_v, q_v, s_v, p_v, seen_v, kbuf, vbuf,
           part_bufs, late_bufs, wsem, ksem, vsem, send_sem, recv_sem):
    me = lax.axis_index("tp")
    peers = {k: other(me, k) for k in range(1, N)}
    mine = pl.ds(pl.multiple_of(me * HEAD, HEAD), HEAD)

    small = [pltpu.make_async_copy(src, dst, wsem.at[i]) for i, (src, dst) in enumerate((
        (x_hbm, x_v), (ga_hbm, ga_v), (wq_hbm, wq_v), (rot_hbm, rot_v)))]
    middle = [pltpu.make_async_copy(src, dst, wsem.at[7 + i]) for i, (src, dst) in enumerate(((wo_hbm, wo_v), (gm_hbm, gm_v)))]
    later = [pltpu.make_async_copy(src, dst, wsem.at[4 + i]) for i, (src, dst) in enumerate((
        (wg_hbm, wg_v), (wu_hbm, wu_v), (wd_hbm, wd_v)))]

    def keys_copy(g):
        slot = lax.rem(g, SLOTS)
        return pltpu.make_async_copy(k_hbm.at[pl.ds(g * GROUP, GROUP)], kbuf.at[slot], ksem.at[slot])

    def values_copy(g):
        slot = lax.rem(g, SLOTS)
        return pltpu.make_async_copy(v_hbm.at[pl.ds(g * GROUP, GROUP)], vbuf.at[slot], vsem.at[slot])

    for copy in small:
        copy.start()
    keys_copy(0).start()
    keys_copy(1).start()
    values_copy(0).start()
    keys_copy(2).start()
    values_copy(1).start()

    barrier = pltpu.get_barrier_semaphore()
    for k in range(1, N):
        pl.semaphore_signal(barrier, inc=1, device_id={"tp": peers[k]}, device_id_type=pl.DeviceIdType.MESH)

    def norm_into(first, rows, columns, gain_v):
        total = jnp.zeros((rows, HEAD), F32)
        for c in range(N):
            wide = columns(c).astype(F32)
            total += wide * wide
        scale = lax.rsqrt(jnp.sum(total, -1, keepdims=True) / D + EPS)
        gain = gain_v[...].astype(F32)
        for c in range(N):
            a_v[first:first + rows, c * HEAD:(c + 1) * HEAD] = (columns(c).astype(F32) * scale * gain[c:c + 1, :]).astype(BF16)

    for copy in small:
        copy.wait()
    norm_into(0, BATCH, lambda c: x_v[:, c * HEAD:(c + 1) * HEAD], ga_v)
    q = jnp.dot(a_v[...], wq_v[...], preferred_element_type=F32).astype(BF16).astype(F32)
    q = q * rot_v[0:1, :] + pltpu.roll(q, HEAD // 2, 1) * rot_v[1:2, :]
    q = q.astype(BF16).astype(F32)
    for g in range(GROUPS):
        q_v[g, :GROUP] = q[g * GROUP:(g + 1) * GROUP]

    for copy in middle:
        copy.start()

    rows = lax.broadcasted_iota(jnp.int32, (ROWS, HEAD), 0)

    def score(g):
        slot = lax.rem(g, SLOTS)
        query = q_v[g]
        own = [jnp.where(rows == i, query, 0.0) for i in range(GROUP)]
        lhs = [jnp.concatenate(own[i:i + 2], 1).astype(BF16) for i in range(0, GROUP, 2)]
        for j in range(TILES):
            keys = slice(j * TILE, (j + 1) * TILE)
            total = None
            for i in range(0, GROUP, 2):
                rhs = jnp.concatenate([kbuf[slot, i, keys, :], kbuf[slot, i + 1, keys, :]], 1)
                part = lax.dot_general(lhs[i // 2], rhs, (((1,), (1,)), ((), ())), preferred_element_type=F32)
                total = part if total is None else total + part
            s_v[:, keys] = total

    def weigh(g):
        scores = s_v[...] * HEAD**-0.5
        e = jnp.exp(scores - jnp.max(scores, -1, keepdims=True))
        p_v[lax.rem(g, 2)] = (e * (1.0 / jnp.sum(e, -1, keepdims=True))).astype(BF16)

    def gather(g):
        slot, place = lax.rem(g, SLOTS), lax.rem(g, 2)
        seen = jnp.zeros((ROWS, HEAD), F32)
        for i in range(0, GROUP, 2):
            out = None
            for j in range(TILES):
                keys = slice(j * TILE, (j + 1) * TILE)
                rhs = jnp.concatenate([vbuf[slot, i, keys, :], vbuf[slot, i + 1, keys, :]], 1)
                part = jnp.dot(p_v[place, :, keys], rhs, preferred_element_type=F32)
                out = part if out is None else out + part
            seen = jnp.where(rows == i, out[:, :HEAD], jnp.where(rows == i + 1, out[:, HEAD:], seen))
        seen_v[g] = seen

    def copy(phase, k, source, target):
        return pltpu.make_async_remote_copy(
            src_ref=source, dst_ref=target, send_sem=send_sem.at[phase], recv_sem=recv_sem.at[phase],
            device_id={"tp": peers[k]}, device_id_type=pl.DeviceIdType.MESH)

    def start(phase, source, target):
        for k in ORDER:
            copy(phase, k, source(k), target(k)).start()

    def arrived(phase, size):
        copy(phase, 1, size, size).wait_recv()

    def left_here(phase, size):
        copy(phase, 1, size, size).wait_send()

    late_send, late_recv, late_send_m, late_recv_m, late_h, late_hidden = late_bufs

    def seen_rows(first, count):
        return jnp.concatenate([seen_v[g, :GROUP] for g in range(first // GROUP, (first + count) // GROUP)], 0).astype(BF16)

    def hidden_rows(first, count, columns, hidden_v):
        norm_into(first, count, columns, gm_v)
        a = a_v[first:first + count]
        gate = jnp.dot(a, wg_v[...], preferred_element_type=F32)
        up = jnp.dot(a, wu_v[...], preferred_element_type=F32)
        hidden_v[...] = (gate * (1.0 / (1.0 + jnp.exp(-gate))) * up).astype(BF16)

    def early_terms(phase, left, w_v, send, recv):
        for c in range(0, N, 2):
            term = jnp.dot(left, w_v[:, c * HEAD:(c + 2) * HEAD], preferred_element_type=F32).astype(BF16)
            send[c] = term[:, :HEAD]
            send[c + 1] = term[:, HEAD:]
        start(phase, lambda k: send.at[peers[k]], lambda k: recv.at[k])

    def early_sum(phase, left, w_v, recv, base):
        total = base + jnp.dot(left, w_v[:, mine], preferred_element_type=F32)
        arrived(phase, recv.at[:N - 1])
        for k in range(1, N):
            total += recv[k].astype(F32)
        return total.astype(BF16)

    def early_a(i):
        early_terms(4 * i, seen_rows(*PARTS[i]), wo_v, part_bufs[i][0], part_bufs[i][1])

    def early_b(i):
        first, rows = PARTS[i]
        h = part_bufs[i][4]
        h[me] = early_sum(4 * i, seen_rows(first, rows), wo_v, part_bufs[i][1], x_v[first:first + rows, mine].astype(F32))
        start(4 * i + 1, lambda k: h.at[me], lambda k: h.at[me])

    def early_c(i):
        first, rows = PARTS[i]
        h, hidden = part_bufs[i][4:]
        arrived(4 * i + 1, h.at[:N - 1])
        hidden_rows(first, rows, lambda c: h[c], hidden)
        early_terms(4 * i + 2, hidden[...], wd_v, part_bufs[i][2], part_bufs[i][3])

    def early_d(i):
        first, rows = PARTS[i]
        block = o_ref.at[first:first + rows, mine]
        block[...] = early_sum(4 * i + 2, part_bufs[i][5][...], wd_v, part_bufs[i][3], part_bufs[i][4][me].astype(F32))
        start(4 * i + 3, lambda k: block, lambda k: block)

    def early_size(i, phase):
        first, rows = PARTS[i]
        return o_ref.at[first:first + rows, :(N - 1) * HEAD] if phase == 3 else part_bufs[i][1].at[:N - 1]

    def early_e(i):
        arrived(4 * i + 3, early_size(i, 3))

    def owns(half):
        a, b, c, d = (me == owner for owner in OWNERS[half])
        return jnp.logical_or(jnp.logical_or(a, b), jnp.logical_or(c, d))

    def by_role(half, job, ref):
        @pl.when(owns(half))
        def _():
            job(ref(len(OWNERS[half]) - 1))

        @pl.when(jnp.logical_not(owns(half)))
        def _():
            job(ref(len(OWNERS[half])))

    def late_terms(half, left, w_v, send, recv):
        for w, owner in enumerate(OWNERS[half]):
            for c in range(0, PART, 2 * HEAD):
                at = w * PART + c
                send[w, :, c:c + 2 * HEAD] = jnp.dot(left, w_v[:, at:at + 2 * HEAD], preferred_element_type=F32).astype(BF16)

            @pl.when(me != owner)
            def _():
                pltpu.make_async_remote_copy(
                    src_ref=send.at[w], dst_ref=recv.at[other(me, owner)], send_sem=send_sem.at[LATE_AT + 2 * half],
                    recv_sem=recv_sem.at[LATE_AT + 2 * half], device_id={"tp": owner}, device_id_type=pl.DeviceIdType.MESH).start()

    def late_sum(half, left, w_v, recv, base, block):
        for w, owner in enumerate(OWNERS[half]):
            @pl.when(me == owner)
            def _():
                total = base(w) + jnp.dot(left, w_v[:, w * PART:(w + 1) * PART], preferred_element_type=F32)
                arrived(LATE_AT + 2 * half, recv.at[:N - 1])
                for k in range(1, N):
                    total += recv[k].astype(F32)
                block(w)[...] = total.astype(BF16)
                order = ORDER if half == 0 else sorted(ORDER, key=lambda k: bin((owner ^ k) >> 1).count("1") * 2 + (owner ^ k) % 2)
                for k in order:
                    copy(LATE_AT + 1 + 2 * half, k, block(w), block(w)).start()

    def late_a():
        late_terms(0, seen_rows(EARLY, LATE), wo_v, late_send, late_recv)

    def late_b():
        late_sum(0, seen_rows(EARLY, LATE), wo_v, late_recv, lambda w: x_v[EARLY:, w * PART:(w + 1) * PART].astype(F32), lambda w: late_h.at[w])

    def late_c():
        by_role(0, lambda size: arrived(LATE_AT + 1, size), lambda n: late_h.at[:n])
        per = PART // HEAD
        hidden_rows(EARLY, LATE, lambda c: late_h[c // per, :, c % per * HEAD:(c % per + 1) * HEAD], late_hidden)
        late_terms(1, late_hidden[...], wd_v, late_send_m, late_recv_m)

    def late_d():
        late_sum(1, late_hidden[...], wd_v, late_recv_m, lambda w: late_h[w].astype(F32), lambda w: o_ref.at[EARLY:, w * PART:(w + 1) * PART])

    def late_e():
        by_role(1, lambda size: arrived(LATE_AT + 3, size), lambda n: o_ref.at[EARLY:, :n * PART])

    keys_copy(0).wait()
    score(0)
    weigh(0)

    def entered():
        for c in middle:
            c.wait()
        pl.semaphore_wait(barrier, N - 1)

    def weights():
        for c in later:
            c.wait()

    stages = {5: (entered,), 7: (lambda: early_a(0),), 9: (lambda: early_b(0),), 11: (weights, lambda: early_c(0)),
              13: (lambda: early_a(1), lambda: early_d(0))}

    def step(g, _):
        keys_copy(g + 1).wait()
        values_copy(g).wait()

        @pl.when(g + 3 < GROUPS)
        def _():
            keys_copy(g + 3).start()

        @pl.when(g + 2 < GROUPS)
        def _():
            values_copy(g + 2).start()

        @pl.when(g == WEIGHTS_AT)
        def _():
            for c in later:
                c.start()

        score(g + 1)
        gather(g)
        weigh(g + 1)

        for when, jobs in stages.items():
            @pl.when(g == when)
            def _():
                for job in jobs:
                    job()

        return 0

    lax.fori_loop(0, GROUPS - 1, step, 0)
    values_copy(GROUPS - 1).wait()
    gather(GROUPS - 1)
    late_a()
    early_b(1)
    late_b()
    early_c(1)
    late_c()
    early_d(1)
    late_d()
    early_e(0)
    early_e(1)
    late_e()

    for i in range(len(PARTS)):
        for phase in range(4):
            left_here(4 * i + phase, early_size(i, phase))
    for half, send, recv in ((0, late_send, late_recv), (1, late_send_m, late_recv_m)):
        by_role(half, lambda size: left_here(LATE_AT + 2 * half, size), lambda n: send.at[:n])

        @pl.when(owns(half))
        def _():
            left_here(LATE_AT + 1 + 2 * half, recv.at[:N - 1])


def rotary_table():
    half = HEAD // 2
    angle = (CACHE - 1) * THETA ** (-np.arange(half, dtype=np.float64) / half)
    cos, sin = np.cos(angle), np.sin(angle)
    table = np.zeros((8, HEAD), np.float32)
    table[0], table[1] = np.concatenate([cos, cos]), np.concatenate([-sin, sin])
    return table


def solution(mesh):
    def step(x, k_cache, v_cache, gain_a, wq, wo, gain_m, w_gate, w_up, w_down):
        whole = pl.BlockSpec(memory_space=pl.ANY)
        call = pl.pallas_call(
            kernel,
            out_shape=jax.ShapeDtypeStruct((BATCH, D), BF16),
            in_specs=[whole] * 11,
            out_specs=pl.BlockSpec(memory_space=pltpu.VMEM),
            scratch_shapes=[
                pltpu.VMEM((BATCH, D), BF16), pltpu.VMEM((N, HEAD), BF16), pltpu.VMEM((N, HEAD), BF16),
                pltpu.VMEM((D, HEAD), BF16), pltpu.VMEM((HEAD, D), BF16), pltpu.VMEM((D, FF), BF16), pltpu.VMEM((D, FF), BF16),
                pltpu.VMEM((FF, D), BF16), pltpu.VMEM((8, HEAD), F32), pltpu.VMEM((BATCH, D), BF16), pltpu.VMEM((GROUPS, ROWS, HEAD), F32),
                pltpu.VMEM((ROWS, CACHE), F32), pltpu.VMEM((2, ROWS, CACHE), BF16), pltpu.VMEM((GROUPS, ROWS, HEAD), F32),
                pltpu.VMEM((SLOTS, GROUP, CACHE, HEAD), BF16), pltpu.VMEM((SLOTS, GROUP, CACHE, HEAD), BF16),
                [[pltpu.VMEM((N, rows, HEAD), BF16)] * 5 + [pltpu.VMEM((rows, FF), BF16)] for _, rows in PARTS],
                [pltpu.VMEM((n, LATE, PART), BF16) for n in (4, N, 4, N, 4)] + [pltpu.VMEM((LATE, FF), BF16)],
                pltpu.SemaphoreType.DMA((9,)), pltpu.SemaphoreType.DMA((SLOTS,)), pltpu.SemaphoreType.DMA((SLOTS,)),
                pltpu.SemaphoreType.DMA((PHASES,)), pltpu.SemaphoreType.DMA((PHASES,)),
            ],
            compiler_params=pltpu.CompilerParams(collective_id=0, has_side_effects=True, vmem_limit_bytes=60 * 2**20),
            name="decode_layer",
        )
        return call(x, k_cache.reshape(BATCH, CACHE, HEAD), v_cache.reshape(BATCH, CACHE, HEAD), gain_a.reshape(N, HEAD), wq, wo,
                    gain_m.reshape(N, HEAD), w_gate, w_up, w_down, jnp.asarray(rotary_table()))

    states, cache, columns, rows_of = P("dp", None), P("dp", None, "tp", None), P(None, "tp"), P("tp", None)
    return jax.shard_map(
        step,
        mesh=mesh,
        in_specs=(states, cache, cache, P(None), columns, rows_of, P(None), columns, columns, rows_of),
        out_specs=states,
        check_vma=False,
    )
```
